32 devices in a mesh: dp: 1 (over z), eo: 4 (over y), em: 4 (over x), ei: 2 (over core).
Axes of the slice: x: 4, y: 4, z: 1, core: 2. Of those that a mesh axis runs over, the one named last changes fastest.
The devices are a block of a 4x4x8 slice.
Arguments:
- x_disp: bfloat16 [32, 64, 24, 2048], P('dp', ('eo', 'em', 'ei'))
- w_gate: bfloat16 [64, 2048, 1408], P(('eo', 'em', 'ei'))
- w_up: bfloat16 [64, 2048, 1408], P(('eo', 'em', 'ei'))
- w_down: bfloat16 [64, 1408, 2048], P(('eo', 'em', 'ei'))
- slot_idx: int32 [4096, 6], P(('dp', 'eo', 'em', 'ei'))
- expert_idx: int32 [4096, 6], P(('dp', 'eo', 'em', 'ei'))
- gate_wt: float32 [4096, 6], P(('dp', 'eo', 'em', 'ei'))
Outputs:
- output: bfloat16 [4096, 2048], P(('dp', 'eo', 'em', 'ei'))
All inputs are finite; a program needn't handle non-finite values.
Results may differ from the reference program's by a relative error of at most 0.00133.
Values are sent between devices in bfloat16 or wider.
A program may use at most 768 MiB of HBM per device.

```python
import jax
import jax.numpy as jnp
from jax import lax

D = 2048
FF = 1408
EXPERTS = 64
TOP = 6
TOK_DEV = 128
GROUP = 32
SLOTS = 24
TOKENS = GROUP * TOK_DEV


def assign_slots(flat_ids):
    sort_order = jnp.argsort(flat_ids, stable=True)
    sorted_ids = flat_ids[sort_order]
    counts = jnp.bincount(flat_ids, length=EXPERTS)
    starts = jnp.cumsum(counts) - counts
    rank_sorted = jnp.arange(TOK_DEV * TOP) - starts[sorted_ids]
    slot_rank = jnp.zeros_like(rank_sorted).at[sort_order].set(rank_sorted)
    return jnp.where(slot_rank < SLOTS, slot_rank, -1).astype(jnp.int32)


def draw_routing(route_key):
    noise_key, bias_key, hot_key, shift_key = jax.random.split(route_key, 4)
    expert_ids = jnp.arange(EXPERTS, dtype=jnp.int32)
    popularity = jax.random.randint(bias_key, (EXPERTS,), 0, 48, dtype=jnp.int32)
    hot_expert = jax.random.randint(hot_key, (), 0, EXPERTS, dtype=jnp.int32)
    popularity = jnp.where(expert_ids == hot_expert, 100000, popularity)
    score_noise = jax.random.randint(noise_key, (TOKENS, EXPERTS), 0, 64, dtype=jnp.int32)
    route_score = (score_noise + popularity[None, :]) * EXPERTS + expert_ids[None, :]
    chosen = lax.top_k(route_score, TOP)[1]
    col_shift = jax.random.randint(shift_key, (TOKENS, 1), 0, TOP, dtype=jnp.int32)
    column = (jnp.arange(TOP, dtype=jnp.int32)[None, :] + col_shift) % TOP
    chosen = jnp.take_along_axis(chosen, column, axis=1).astype(jnp.int32)
    slot_idx = jax.vmap(assign_slots)(chosen.reshape(GROUP, TOK_DEV * TOP))
    return slot_idx.reshape(TOKENS, TOP), chosen


def setup_inputs(seed: int = 0, part: int = 0) -> dict:
    part_key = jax.random.fold_in(jax.random.key(seed), part)
    x_key, route_key, gate_key = jax.random.split(part_key, 3)
    wg_key, wu_key, wd_key = jax.random.split(jax.random.key(seed + 1), 3)
    x_disp = jax.random.normal(x_key, (GROUP, EXPERTS, SLOTS, D), jnp.float32).astype(jnp.bfloat16)
    w_gate = (jax.random.normal(wg_key, (EXPERTS, D, FF), jnp.float32) * D ** -0.5).astype(jnp.bfloat16)
    w_up = (jax.random.normal(wu_key, (EXPERTS, D, FF), jnp.float32) * D ** -0.5).astype(jnp.bfloat16)
    w_down = (jax.random.normal(wd_key, (EXPERTS, FF, D), jnp.float32) * (1.5 * FF ** -0.5)).astype(jnp.bfloat16)
    slot_idx, expert_idx = draw_routing(route_key)
    gate_wt = jax.nn.softmax(1.2 * jax.random.normal(gate_key, (TOKENS, TOP), jnp.float32), axis=-1)
    return {'x_disp': x_disp, 'w_gate': w_gate, 'w_up': w_up, 'w_down': w_down,
            'slot_idx': slot_idx, 'expert_idx': expert_idx, 'gate_wt': gate_wt}


def reference(x_disp, w_gate, w_up, w_down, slot_idx, expert_idx, gate_wt):
    def expert_rows(operands):
        x_rows, wg_e, wu_e, wd_e = operands
        flat_rows = x_rows.reshape(GROUP * SLOTS, D)
        gate_pre = jnp.dot(flat_rows, wg_e, preferred_element_type=jnp.float32)
        up_pre = jnp.dot(flat_rows, wu_e, preferred_element_type=jnp.float32)
        hidden = (jax.nn.silu(gate_pre) * up_pre).astype(jnp.bfloat16)
        y_flat = jnp.dot(hidden, wd_e, preferred_element_type=jnp.float32).astype(jnp.bfloat16)
        return y_flat.reshape(GROUP, SLOTS, D)

    y_rows = lax.map(expert_rows, (jnp.swapaxes(x_disp, 0, 1), w_gate, w_up, w_down))
    source = (jnp.arange(TOKENS, dtype=jnp.int32) // TOK_DEV)[:, None]
    is_live = slot_idx >= 0
    row_index = jnp.where(is_live, (expert_idx * GROUP + source) * SLOTS + slot_idx, 0)
    weight = jnp.where(is_live, gate_wt, 0.0)
    picked = jnp.take(y_rows.reshape(EXPERTS * GROUP * SLOTS, D), row_index, axis=0)
    combined = jnp.sum(weight[:, :, None] * picked.astype(jnp.float32), axis=1)
    return combined.astype(jnp.bfloat16)
```

```python
import functools

import jax
import jax.numpy as jnp
from jax import lax
from jax.experimental import pallas as pl
from jax.experimental.pallas import tpu as pltpu
from jax.sharding import PartitionSpec as P

GROUP_AXES = ('eo', 'em', 'ei')
MESH = pl.DeviceIdType.MESH
TILE = 256
ROUTE_ROWS = 8


def kernel(n, cores, slots, top, x_hbm, wg_hbm, wu_hbm, wd_hbm, route_ref, out_ref,
           wg, wu, wl, wd, xs, xe, hid, ybuf, recv, part, prec, own, routes,
           gu_sem, wl_sem, wd_sem, x_sem, s1, r1, s2, r2, s3, r3):
    experts, model, ff = wg_hbm.shape
    ff_main = wg.shape[2]
    half = ff - ff_main
    rows = experts * slots
    tokens = out_ref.shape[0]
    y, x, c = (lax.axis_index(a) for a in GROUP_AXES)

    def wrap(v):
        return lax.rem(v, n)

    barrier = pltpu.get_barrier_semaphore()
    for oy in range(n):
        for ox in range(n):
            for oc in range(cores):
                if oy or ox or oc:
                    pl.semaphore_signal(barrier, inc=1, device_id_type=MESH, device_id={
                        'eo': wrap(y + oy), 'em': wrap(x + ox), 'ei': lax.rem(c + oc, cores)})

    def x_copies(i):
        step = wrap(i + 1)
        buf = lax.rem(i, 2)
        out = []
        for t in range(2):
            for j in range(n):
                if t == 0:
                    src = (wrap(y + step) * n + wrap(x + j)) * cores
                else:
                    src = (wrap(y + j) * n + wrap(x + step)) * cores + 1
                d = t * n + j
                out.append(pltpu.make_async_copy(x_hbm.at[src], xs.at[buf, d], x_sem.at[buf, d]))
        return out

    main_tiles = ff_main // TILE

    def gate_up_copies(e, k):
        if k < main_tiles:
            cols = pl.ds(k * TILE, TILE)
            return [pltpu.make_async_copy(w.at[e, :, cols], v.at[e, :, cols], gu_sem.at[e, k, a])
                    for a, (w, v) in enumerate(((wg_hbm, wg), (wu_hbm, wu)))]
        cols = pl.ds(ff_main, half)
        return [pltpu.make_async_copy(w.at[e, :, cols], wl.at[e, :, pl.ds(a * half, half)], wl_sem.at[e, a])
                for a, w in enumerate((wg_hbm, wu_hbm))]

    def down_copies(e, k):
        cols = pl.ds(k * TILE, TILE)
        return [pltpu.make_async_copy(wd_hbm.at[e, :, cols], wd.at[e, :, cols], wd_sem.at[e, k])]

    down_tiles = model // TILE
    for cp in x_copies(0):
        cp.start()
    for e in range(experts):
        for k in range(main_tiles + 1):
            for cp in gate_up_copies(e, k):
                cp.start()
    for k in range(down_tiles):
        for e in range(experts):
            for cp in down_copies(e, k):
                cp.start()

    def compute(i, first):
        buf = lax.rem(i, 2)
        for cp in x_copies(i):
            cp.wait()
        for k in range(0, model, 2 * TILE):
            cols = pl.ds(k, 2 * TILE)
            pieces = [xs[buf, d, :, cols].astype(jnp.float32) for d in range(2 * n)]
            for e in range(experts):
                xe[e, :, cols] = jnp.concatenate(
                    [p[e * slots:(e + 1) * slots] for p in pieces], axis=0).astype(jnp.bfloat16)
        for e in range(experts):
            for k in range(main_tiles + 1):
                if first:
                    for cp in gate_up_copies(e, k):
                        cp.wait()
                if k < main_tiles:
                    cols = pl.ds(k * TILE, TILE)
                    g = jnp.dot(xe[e], wg[e, :, cols], preferred_element_type=jnp.float32)
                    u = jnp.dot(xe[e], wu[e, :, cols], preferred_element_type=jnp.float32)
                    hid[e, :, cols] = (jax.nn.silu(g) * u).astype(jnp.bfloat16)
                else:
                    gu = jnp.dot(xe[e], wl[e], preferred_element_type=jnp.float32)
                    hid[e, :, pl.ds(ff_main, half)] = (
                        jax.nn.silu(gu[:, :half]) * gu[:, half:]).astype(jnp.bfloat16)
        for k in range(down_tiles):
            cols = pl.ds(k * TILE, TILE)
            if first:
                for e in range(experts):
                    for cp in down_copies(e, k):
                        cp.wait()
            ys = [jnp.dot(hid[e], wd[e, :, cols], preferred_element_type=jnp.float32) for e in range(experts)]
            for d in range(2 * n):
                block = jnp.concatenate([v[d * slots:(d + 1) * slots] for v in ys], axis=0)
                ybuf[i, d // n, d % n, :, cols] = block.astype(jnp.bfloat16)

    ring = jnp.where(c == 0, x, y)

    def row_sends(i):
        out = []
        for j in range(1, n):
            out.append(pltpu.make_async_remote_copy(
                src_ref=ybuf.at[i, 0, j], dst_ref=recv.at[i, x, c], send_sem=s1.at[i, 0, j],
                recv_sem=r1.at[i, x, c], device_id={'eo': y, 'em': wrap(x + j), 'ei': 0}, device_id_type=MESH))
            out.append(pltpu.make_async_remote_copy(
                src_ref=ybuf.at[i, 1, j], dst_ref=recv.at[i, y, c], send_sem=s1.at[i, 1, j],
                recv_sem=r1.at[i, y, c], device_id={'eo': wrap(y + j), 'em': x, 'ei': 1}, device_id_type=MESH))
        other = 1 - c
        q = jnp.where(c == 0, y, x)
        out.append(pltpu.make_async_remote_copy(
            src_ref=ybuf.at[i, other, 0], dst_ref=recv.at[i, q, c], send_sem=s1.at[i, other, 0],
            recv_sem=r1.at[i, q, c], device_id={'eo': y, 'em': x, 'ei': other}, device_id_type=MESH))
        return out

    def wait_rows(i):
        def one(q, cc):
            pltpu.make_async_remote_copy(
                src_ref=ybuf.at[i, 0, 0], dst_ref=recv.at[i, q, cc], send_sem=s1.at[i, 0, 0],
                recv_sem=r1.at[i, q, cc], device_id={'eo': y, 'em': x, 'ei': 1 - c},
                device_id_type=MESH).wait_recv()
        one(ring, 1 - c)
        for j in range(1, n):
            for cc in range(cores):
                one(wrap(ring + j), cc)

    def send_rows(i):
        for cp in row_sends(i):
            cp.start()
        recv[i, ring, c] = ybuf[i, c, 0]

    along_y = jnp.where(c == 0, 1, 0)

    def ahead(step):
        return {'eo': wrap(y + step * along_y), 'em': wrap(x + step * (1 - along_y)), 'ei': c}

    def part_send(i):
        return pltpu.make_async_remote_copy(
            src_ref=part.at[i], dst_ref=prec.at[i], send_sem=s2.at[i], recv_sem=r2.at[i],
            device_id=ahead(i + 1), device_id_type=MESH)

    def route_send(i):
        return pltpu.make_async_remote_copy(
            src_ref=route_ref, dst_ref=routes.at[i], send_sem=s3.at[i], recv_sem=r3.at[i],
            device_id=ahead(n - 1 - i), device_id_type=MESH)

    def combine(i, route, store):
        taken = n * cores * rows
        r = lax.broadcasted_iota(jnp.int32, (taken, tokens), 0)
        q = sum((r >= m * cores * rows).astype(jnp.int32) for m in range(1, n))
        chip = cores * experts
        base = jnp.where(c == 0, y * (n * chip), x * chip) * slots
        jump = jnp.where(c == 0, 0, (n - 1) * chip * slots)
        key = (base + r + q * jump).astype(jnp.float32)
        weight = jnp.zeros((taken, tokens), jnp.float32)
        for j in range(top):
            weight = weight + jnp.where(route[j:j + 1, :] == key, route[ROUTE_ROWS + j:ROUTE_ROWS + j + 1, :], 0.0)
        live = jnp.max(weight, axis=1, keepdims=True) > 0
        hi = weight.astype(jnp.bfloat16)
        rest = weight - hi.astype(jnp.float32)
        mid = rest.astype(jnp.bfloat16)
        low = (rest - mid.astype(jnp.float32)).astype(jnp.bfloat16)
        lhs = jnp.concatenate([hi, mid, low], axis=1)
        for k in range(down_tiles):
            cols = pl.ds(k * TILE, TILE)
            got = recv[i, :, :, :, cols].reshape(taken, TILE)
            got = jnp.where(live, got.astype(jnp.float32), 0.0).astype(jnp.bfloat16)
            p = lax.dot_general(lhs, got, (((0,), (0,)), ((), ())), preferred_element_type=jnp.float32)
            store(cols, (p[2 * tokens:] + p[tokens:2 * tokens]) + p[:tokens])

    compute(0, True)
    for cp in x_copies(1):
        cp.start()
    pl.semaphore_wait(barrier, n * n * cores - 1)
    send_rows(0)
    for i in range(n - 1):
        route_send(i).start()
    for i in range(n - 1):
        route_send(i).wait_recv()

    @pl.loop(1, n)
    def _(i):
        compute(i, False)
        send_rows(i)

        @pl.when(i < n - 1)
        def _():
            for cp in x_copies(i + 1):
                cp.start()

        prev = i - 1
        wait_rows(prev)

        def store(cols, value):
            part[prev, :, cols] = value

        combine(prev, routes[prev], store)
        part_send(prev).start()

    wait_rows(n - 1)

    def store(cols, value):
        own[:, cols] = value

    combine(n - 1, route_ref[...], store)
    for i in range(n - 1):
        part_send(i).wait_recv()
    for k in range(down_tiles):
        cols = pl.ds(k * TILE, TILE)
        total = own[:, cols]
        for i in range(n - 1):
            total = total + prec[i, :, cols]
        out_ref[:, cols] = total.astype(out_ref.dtype)
    for i in range(n - 1):
        part_send(i).wait_send()
        route_send(i).wait_send()

    @pl.loop(0, n)
    def _(i):
        for cp in row_sends(i):
            cp.wait_send()


def solution(mesh):
    token_spec = P(('dp',) + GROUP_AXES, None)
    weight_spec = P(GROUP_AXES, None, None)
    rows_spec = P('dp', GROUP_AXES, None, None)
    n, cores = mesh.shape['eo'], mesh.shape['ei']
    assert mesh.shape['em'] == n and cores == 2

    def local_part(x_local, w_gate, w_up, w_down, slot_idx, expert_idx, gate_wt):
        sources, experts, slots, model = x_local.shape
        ff = w_gate.shape[2]
        tokens, top = slot_idx.shape
        ff_main = ff // TILE * TILE
        half = ff - ff_main
        assert 2 * half == TILE
        key = jnp.where(slot_idx >= 0, expert_idx * slots + slot_idx, -1).astype(jnp.float32)
        pad = ((0, ROUTE_ROWS - top), (0, 0))
        route = jnp.concatenate([jnp.pad(key.T, pad, constant_values=-1.0), jnp.pad(gate_wt.T, pad)], axis=0)
        rows = experts * slots
        chunk = 2 * n
        hbm = pl.BlockSpec(memory_space=pl.ANY)
        vmem = pl.BlockSpec(memory_space=pltpu.VMEM)
        dma = pltpu.SemaphoreType.DMA
        return pl.pallas_call(
            functools.partial(kernel, n, cores, slots, top),
            out_shape=jax.ShapeDtypeStruct((tokens, model), jnp.bfloat16),
            in_specs=[hbm, hbm, hbm, hbm, vmem],
            out_specs=vmem,
            scratch_shapes=[
                pltpu.VMEM((experts, model, ff_main), jnp.bfloat16),
                pltpu.VMEM((experts, model, ff_main), jnp.bfloat16),
                pltpu.VMEM((experts, model, 2 * half), jnp.bfloat16),
                pltpu.VMEM((experts, ff, model), jnp.bfloat16),
                pltpu.VMEM((2, chunk, rows, model), jnp.bfloat16),
                pltpu.VMEM((experts, chunk * slots, model), jnp.bfloat16),
                pltpu.VMEM((experts, chunk * slots, ff), jnp.bfloat16),
                pltpu.VMEM((n, 2, n, rows, model), jnp.bfloat16),
                pltpu.VMEM((n, n, cores, rows, model), jnp.bfloat16),
                pltpu.VMEM((n - 1, tokens, model), jnp.float32),
                pltpu.VMEM((n - 1, tokens, model), jnp.float32),
                pltpu.VMEM((tokens, model), jnp.float32),
                pltpu.VMEM((n - 1, 2 * ROUTE_ROWS, tokens), jnp.float32),
                dma((experts, ff_main // TILE, 2)), dma((experts, 2)), dma((experts, model // TILE)), dma((2, chunk)),
                dma((n, 2, n)), dma((n, n, cores)), dma((n - 1,)), dma((n - 1,)), dma((n - 1,)), dma((n - 1,)),
            ],
            compiler_params=pltpu.CompilerParams(
                collective_id=0, has_side_effects=True, vmem_limit_bytes=67_000_000),
        )(x_local.reshape(sources, rows, model), w_gate, w_up, w_down, route)

    return jax.shard_map(local_part, mesh=mesh,
                         in_specs=(rows_spec, weight_spec, weight_spec, weight_spec, token_spec, token_spec, token_spec),
                         out_specs=token_spec, check_vma=False)
```

```python
import functools

import jax
import jax.numpy as jnp
from jax import lax
from jax.experimental import pallas as pl
from jax.experimental.pallas import tpu as pltpu
from jax.sharding import PartitionSpec as P

GROUP_AXES = ('eo', 'em', 'ei')
MESH = pl.DeviceIdType.MESH
TILE = 256
DOWN_TILE = 512
ROUTE_ROWS = 8
PAIR = (1, 3)
SINGLE = (2, 0)


def kernel(n, cores, slots, top, x_hbm, wg_hbm, wu_hbm, wd_hbm, slot_hbm, expert_hbm, gate_hbm, out_ref,
           wg, wu, wl, wd, xs, xe, hid, ybuf, recv, part, prec, own, slot_ref, expert_ref, gate_ref, packed, routes,
           gu_sem, wl_sem, wd_sem, x_sem, route_sem, s1, r1, s2, r2, s3, r3):
    experts, model, ff = wg_hbm.shape
    ff_main = wg.shape[2]
    half = ff - ff_main
    rows = 2 * slots
    blocks = 2 * n
    stages = 2 * experts
    tokens = out_ref.shape[0]
    y, x, c = (lax.axis_index(a) for a in GROUP_AXES)
    ring = jnp.where(c == 0, x, y)
    along_y = jnp.where(c == 0, 1, 0)

    def wrap(v):
        return lax.rem(v, n)

    barrier = pltpu.get_barrier_semaphore()
    for oy in range(n):
        for ox in range(n):
            for oc in range(cores):
                if oy or ox or oc:
                    pl.semaphore_signal(barrier, inc=1, device_id_type=MESH, device_id={
                        'eo': wrap(y + oy), 'em': wrap(x + ox), 'ei': lax.rem(c + oc, cores)})

    def x_copy(t, j, step, d):
        if t == 0:
            src = (wrap(y + step) * n + wrap(x + j)) * cores
        else:
            src = (wrap(y + j) * n + wrap(x + step)) * cores + 1
        return pltpu.make_async_copy(x_hbm.at[src], xs.at[d], x_sem.at[d])

    blocks_in_order = [(t, j) for j in range(n) for t in range(2)]

    def pair_copies():
        return [x_copy(t, j, PAIR[h], (t * n + j) * 2 + h) for t, j in blocks_in_order for h in range(2)]

    def single_copies(i):
        return [x_copy(t, j, SINGLE[i], i * blocks + t * n + j) for t, j in blocks_in_order]

    main_tiles = ff_main // TILE
    down_tiles = model // TILE

    def gate_up_copies(e, k):
        if k < main_tiles:
            cols = pl.ds(k * TILE, TILE)
            return [pltpu.make_async_copy(w.at[e, :, cols], v.at[e, :, cols], gu_sem.at[e, k, a])
                    for a, (w, v) in enumerate(((wg_hbm, wg), (wu_hbm, wu)))]
        cols = pl.ds(ff_main, half)
        return [pltpu.make_async_copy(w.at[e, :, cols], wl.at[e, :, pl.ds(a * half, half)], wl_sem.at[e, a])
                for a, w in enumerate((wg_hbm, wu_hbm))]

    def down_copies(e, k):
        cols = pl.ds(k * TILE, TILE)
        return [pltpu.make_async_copy(wd_hbm.at[e, :, cols], wd.at[e, :, cols], wd_sem.at[e, k])]

    loads = [pltpu.make_async_copy(src, dst, route_sem.at[i]) for i, (src, dst) in enumerate(
        ((slot_hbm, slot_ref), (expert_hbm, expert_ref), (gate_hbm, gate_ref)))]
    for cp in loads:
        cp.start()
    for cp in pair_copies():
        cp.start()
    for e in range(experts):
        for k in range(main_tiles + 1):
            for cp in gate_up_copies(e, k):
                cp.start()
        for k in range(down_tiles):
            for cp in down_copies(e, k):
                cp.start()

    for cp in loads:
        cp.wait()
    slot = slot_ref[...]
    packed[...] = jnp.zeros_like(packed)
    packed[0:top] = jnp.where(slot >= 0, expert_ref[...] * slots + slot, -1).astype(jnp.float32)
    packed[ROUTE_ROWS:ROUTE_ROWS + top] = gate_ref[...]

    def ahead(step):
        return {'eo': wrap(y + step * along_y), 'em': wrap(x + step * (1 - along_y)), 'ei': c}

    def route_send(step):
        return pltpu.make_async_remote_copy(
            src_ref=packed, dst_ref=routes.at[step - 1], send_sem=s3.at[step - 1], recv_sem=r3.at[step - 1],
            device_id=ahead(n - step), device_id_type=MESH)

    def arrange_pair():
        for cp in pair_copies():
            cp.wait()
        for k in range(0, model, TILE):
            cols = pl.ds(k, TILE)
            for b in range(blocks):
                first, second = (xs[2 * b + h, :, cols].astype(jnp.float32) for h in range(2))
                for e in range(experts):
                    part_rows = slice(e * slots, (e + 1) * slots)
                    xe[e, pl.ds(b * rows, rows), cols] = jnp.concatenate(
                        [first[part_rows], second[part_rows]], axis=0).astype(jnp.bfloat16)

    def arrange_single(i):
        for b in range(blocks):
            d = i * blocks + b
            pltpu.make_async_copy(x_hbm.at[0], xs.at[d], x_sem.at[d]).wait()
        for k in range(0, model, TILE):
            cols = pl.ds(k, TILE)
            for b in range(0, blocks, 2):
                first, second = (xs[i * blocks + b + h, :, cols].astype(jnp.float32) for h in range(2))
                for e in range(experts):
                    part_rows = slice(e * slots, (e + 1) * slots)
                    xe[e, pl.ds(b * slots, rows), cols] = jnp.concatenate(
                        [first[part_rows], second[part_rows]], axis=0).astype(jnp.bfloat16)

    def gate_up(e, k, count, at):
        dst = pl.ds(at, count)
        lhs = xe[e, 0:count]
        if k < main_tiles:
            cols = pl.ds(k * TILE, TILE)
            g = jnp.dot(lhs, wg[e, :, cols], preferred_element_type=jnp.float32)
            u = jnp.dot(lhs, wu[e, :, cols], preferred_element_type=jnp.float32)
            hid[dst, cols] = (jax.nn.silu(g) * u).astype(jnp.bfloat16)
        else:
            gu = jnp.dot(lhs, wl[e], preferred_element_type=jnp.float32)
            hid[dst, pl.ds(ff_main, half)] = (jax.nn.silu(gu[:, :half]) * gu[:, half:]).astype(jnp.bfloat16)

    def down_pair(s, e, k):
        cols = pl.ds(k, DOWN_TILE)
        out = jnp.dot(hid[...], wd[e, :, cols], preferred_element_type=jnp.float32).astype(jnp.bfloat16)
        ybuf[s, :, :, cols] = out.reshape(blocks, rows, DOWN_TILE)

    def down_single(s, k):
        cols = pl.ds(k, TILE)
        outs = [jnp.dot(hid[pl.ds(e * blocks * slots, blocks * slots)], wd[e, :, cols],
                        preferred_element_type=jnp.float32) for e in range(experts)]
        for b in range(blocks):
            block = jnp.concatenate([v[b * slots:(b + 1) * slots] for v in outs], axis=0)
            ybuf[s, b, :, cols] = block.astype(jnp.bfloat16)

    def row_sends(s):
        out = []
        for j in range(1, n):
            out.append(pltpu.make_async_remote_copy(
                src_ref=ybuf.at[s, j], dst_ref=recv.at[s, x, c], send_sem=s1.at[s, j],
                recv_sem=r1.at[s, x, c], device_id={'eo': y, 'em': wrap(x + j), 'ei': 0}, device_id_type=MESH))
            out.append(pltpu.make_async_remote_copy(
                src_ref=ybuf.at[s, n + j], dst_ref=recv.at[s, y, c], send_sem=s1.at[s, n + j],
                recv_sem=r1.at[s, y, c], device_id={'eo': wrap(y + j), 'em': x, 'ei': 1}, device_id_type=MESH))
        other = 1 - c
        q = jnp.where(c == 0, y, x)
        out.append(pltpu.make_async_remote_copy(
            src_ref=ybuf.at[s, other * n], dst_ref=recv.at[s, q, c], send_sem=s1.at[s, other * n],
            recv_sem=r1.at[s, q, c], device_id={'eo': y, 'em': x, 'ei': other}, device_id_type=MESH))
        return out

    def send_rows(s):
        for cp in row_sends(s):
            cp.start()
        recv[s, ring, c] = ybuf[s, c * n]

    def wait_rows(s):
        def one(q, cc):
            pltpu.make_async_remote_copy(
                src_ref=ybuf.at[s, 0], dst_ref=recv.at[s, q, cc], send_sem=s1.at[s, 0],
                recv_sem=r1.at[s, q, cc], device_id={'eo': y, 'em': x, 'ei': 1 - c},
                device_id_type=MESH).wait_recv()
        one(ring, 1 - c)
        for j in range(1, n):
            for cc in range(cores):
                one(wrap(ring + j), cc)

    def part_send(step):
        return pltpu.make_async_remote_copy(
            src_ref=part.at[step - 1], dst_ref=prec.at[step - 1], send_sem=s2.at[step - 1], recv_sem=r2.at[step - 1],
            device_id=ahead(step), device_id_type=MESH)

    def combine(order, route, store):
        chip = cores * experts
        base = jnp.where(c == 0, y * (n * chip), x * chip)
        jump = jnp.where(c == 0, chip, n * chip)
        row = lax.broadcasted_iota(jnp.int32, (slots, tokens), 0)
        weights, live = [], []
        for _, q, cc, e, _ in order:
            expert = base + q * jump + cc * experts + e
            key = (row + expert * slots).astype(jnp.float32)
            w = jnp.zeros((slots, tokens), jnp.float32)
            for j in range(top):
                w = w + jnp.where(route[j:j + 1, :] == key, route[ROUTE_ROWS + j:ROUTE_ROWS + j + 1, :], 0.0)
            weights.append(w)
            live.append(jnp.max(w, axis=1, keepdims=True) > 0)
        weight = jnp.concatenate(weights, axis=0)
        hi = weight.astype(jnp.bfloat16)
        rest = weight - hi.astype(jnp.float32)
        mid = rest.astype(jnp.bfloat16)
        low = (rest - mid.astype(jnp.float32)).astype(jnp.bfloat16)
        lhs = jnp.concatenate([hi, mid, low], axis=1)
        for k in range(down_tiles):
            cols = pl.ds(k * TILE, TILE)
            got = []
            for (s, q, cc, _, at), keep in zip(order, live):
                block = recv[s, q, cc, :, cols].astype(jnp.float32)
                got.append(jnp.where(keep, block[at * slots:(at + 1) * slots], 0.0))
            got = jnp.concatenate(got, axis=0).astype(jnp.bfloat16)
            p = lax.dot_general(lhs, got, (((0,), (0,)), ((), ())), preferred_element_type=jnp.float32)
            store(cols, (p[2 * tokens:] + p[tokens:2 * tokens]) + p[:tokens])

    def combine_group(step, order):
        def store(cols, value):
            if step:
                part[step - 1, :, cols] = value
            else:
                own[:, cols] = value

        combine(order, routes[step - 1] if step else packed[...], store)
        if step:
            part_send(step).start()

    senders = [(q, cc) for q in range(n) for cc in range(cores)]

    @pl.loop(0, experts)
    def _(s):
        @pl.when(s == 0)
        def _():
            arrange_pair()
            for i in range(2):
                for cp in single_copies(i):
                    cp.start()

        for m in range(experts):
            @pl.when(s == m)
            def _():
                for k in range(main_tiles + 1):
                    for cp in gate_up_copies(m, k):
                        cp.wait()
        for k in range(main_tiles + 1):
            gate_up(s, k, blocks * rows, 0)
        for m in range(experts):
            @pl.when(s == m)
            def _():
                for k in range(down_tiles):
                    for cp in down_copies(m, k):
                        cp.wait()
        for k in range(0, model, DOWN_TILE):
            down_pair(s, s, k)

        @pl.when(s == 0)
        def _():
            pl.semaphore_wait(barrier, n * n * cores - 1)
            for step in range(1, n):
                route_send(step).start()

        send_rows(s)

    @pl.loop(experts, stages)
    def _(s):
        arrange_single(s - experts)
        for e in range(experts):
            for k in range(main_tiles + 1):
                gate_up(e, k, blocks * slots, e * blocks * slots)
        for k in range(0, model, TILE):
            down_single(s, k)
        send_rows(s)

        @pl.when(s == experts)
        def _():
            for step in range(1, n):
                route_send(step).wait_recv()
            for e in range(experts):
                wait_rows(e)
            for h in range(2):
                combine_group(PAIR[h], [(e, q, cc, e, h) for e in range(experts) for q, cc in senders])

    for i in range(2):
        wait_rows(experts + i)
        combine_group(SINGLE[i], [(experts + i, q, cc, e, e) for q, cc in senders for e in range(experts)])
    for step in range(1, n):
        part_send(step).wait_recv()
    for k in range(down_tiles):
        cols = pl.ds(k * TILE, TILE)
        total = own[:, cols]
        for i in range(n - 1):
            total = total + prec[i, :, cols]
        out_ref[:, cols] = total.astype(out_ref.dtype)
    for step in range(1, n):
        part_send(step).wait_send()
        route_send(step).wait_send()

    @pl.loop(0, stages)
    def _(s):
        for cp in row_sends(s):
            cp.wait_send()


def solution(mesh):
    token_spec = P(('dp',) + GROUP_AXES, None)
    weight_spec = P(GROUP_AXES, None, None)
    rows_spec = P('dp', GROUP_AXES, None, None)
    n, cores = mesh.shape['eo'], mesh.shape['ei']
    assert mesh.shape['em'] == n == 4 and cores == 2

    def local_part(x_local, w_gate, w_up, w_down, slot_idx, expert_idx, gate_wt):
        sources, experts, slots, model = x_local.shape
        ff = w_gate.shape[2]
        tokens, top = slot_idx.shape
        ff_main = ff // TILE * TILE
        half = ff - ff_main
        assert 2 * half == TILE and experts == 2
        rows = 2 * slots
        blocks = 2 * n
        stages = 2 * experts
        hbm = pl.BlockSpec(memory_space=pl.ANY)
        vmem = pl.BlockSpec(memory_space=pltpu.VMEM)
        dma = pltpu.SemaphoreType.DMA
        return pl.pallas_call(
            functools.partial(kernel, n, cores, slots, top),
            out_shape=jax.ShapeDtypeStruct((tokens, model), jnp.bfloat16),
            in_specs=[hbm] * 7,
            out_specs=vmem,
            scratch_shapes=[
                pltpu.VMEM((experts, model, ff_main), jnp.bfloat16),
                pltpu.VMEM((experts, model, ff_main), jnp.bfloat16),
                pltpu.VMEM((experts, model, 2 * half), jnp.bfloat16),
                pltpu.VMEM((experts, ff, model), jnp.bfloat16),
                pltpu.VMEM((2 * blocks, experts * slots, model), jnp.bfloat16),
                pltpu.VMEM((experts, blocks * rows, model), jnp.bfloat16),
                pltpu.VMEM((blocks * rows, ff), jnp.bfloat16),
                pltpu.VMEM((stages, blocks, rows, model), jnp.bfloat16),
                pltpu.VMEM((stages, n, cores, rows, model), jnp.bfloat16),
                pltpu.VMEM((n - 1, tokens, model), jnp.float32),
                pltpu.VMEM((n - 1, tokens, model), jnp.float32),
                pltpu.VMEM((tokens, model), jnp.float32),
                pltpu.VMEM((top, tokens), jnp.int32),
                pltpu.VMEM((top, tokens), jnp.int32),
                pltpu.VMEM((top, tokens), jnp.float32),
                pltpu.VMEM((2 * ROUTE_ROWS, tokens), jnp.float32),
                pltpu.VMEM((n - 1, 2 * ROUTE_ROWS, tokens), jnp.float32),
                dma((experts, ff_main // TILE, 2)), dma((experts, 2)), dma((experts, model // TILE)), dma((2 * blocks,)), dma((3,)),
                dma((stages, blocks)), dma((stages, n, cores)), dma((n - 1,)), dma((n - 1,)), dma((n - 1,)), dma((n - 1,)),
            ],
            compiler_params=pltpu.CompilerParams(
                collective_id=0, has_side_effects=True, vmem_limit_bytes=67_000_000),
        )(x_local.reshape(sources, experts * slots, model), w_gate, w_up, w_down, slot_idx.T, expert_idx.T, gate_wt.T)

    return jax.shard_map(local_part, mesh=mesh,
                         in_specs=(rows_spec, weight_spec, weight_spec, weight_spec, token_spec, token_spec, token_spec),
                         out_specs=token_spec, check_vma=False)
```

```python
import functools

import jax
import jax.numpy as jnp
from jax import lax
from jax.experimental import pallas as pl
from jax.experimental.pallas import tpu as pltpu
from jax.sharding import PartitionSpec as P

GROUP_AXES = ('eo', 'em', 'ei')
MESH = pl.DeviceIdType.MESH
TILE = 256
DOWN_TILE = 512
ROUTE_ROWS = 8
PAIR = (2, 1)
SINGLE = (3, 0)
ORDER = ((0, 1), (1, 1), (0, 3), (1, 3), (0, 2), (1, 2), (0, 0), (1, 0))


def kernel(n, cores, slots, top, x_hbm, wg_hbm, wu_hbm, wd_hbm, slot_hbm, expert_hbm, gate_hbm, out_ref,
           wg, wu, wl, wd, xs, xe, hid, ybuf, recv, part, mid_in, prec, slot_ref, expert_ref, gate_ref, packed, routes,
           gu_sem, wl_sem, wd_sem, x_sem, route_sem, s1, r1, s2, r2, s3, r3, s4, r4):
    experts, model, ff = wg_hbm.shape
    ff_main = wg.shape[2]
    half = ff - ff_main
    rows = 2 * slots
    blocks = 2 * n
    part_blocks = blocks // 2
    stages = 2 * experts
    tokens = out_ref.shape[0]
    y, x, c = (lax.axis_index(a) for a in GROUP_AXES)
    ring = jnp.where(c == 0, x, y)
    along_y = jnp.where(c == 0, 1, 0)

    def wrap(v):
        return lax.rem(v, n)

    def ahead(step):
        return {'eo': wrap(y + step * along_y), 'em': wrap(x + step * (1 - along_y)), 'ei': c}

    def x_copy(t, j, step, d):
        if t == 0:
            src = (wrap(y + step) * n + wrap(x + j)) * cores
        else:
            src = (wrap(y + j) * n + wrap(x + step)) * cores + 1
        return pltpu.make_async_copy(x_hbm.at[src], xs.at[d], x_sem.at[d])

    def pair_copies():
        return [x_copy(t, j, PAIR[h], 2 * p + h) for p, (t, j) in enumerate(ORDER) for h in range(2)]

    def single_copies(i):
        return [x_copy(t, j, SINGLE[i], i * blocks + p) for p, (t, j) in enumerate(ORDER)]

    main_tiles = ff_main // TILE
    down_tiles = model // TILE

    def gate_up_copies(e):
        out = []
        for a, (w, v) in enumerate(((wg_hbm, wg), (wu_hbm, wu))):
            out.append(pltpu.make_async_copy(w.at[e, :, pl.ds(0, ff_main)], v.at[e], gu_sem.at[e, a]))
            out.append(pltpu.make_async_copy(
                w.at[e, :, pl.ds(ff_main, half)], wl.at[e, :, pl.ds(a * half, half)], wl_sem.at[e, a]))
        return out

    def down_copy(e):
        return pltpu.make_async_copy(wd_hbm.at[e], wd.at[e], wd_sem.at[e])

    loads = [pltpu.make_async_copy(src, dst, route_sem.at[i]) for i, (src, dst) in enumerate(
        ((slot_hbm, slot_ref), (expert_hbm, expert_ref), (gate_hbm, gate_ref)))]
    for cp in loads:
        cp.start()
    for cp in pair_copies():
        cp.start()
    for e in range(experts):
        for cp in gate_up_copies(e):
            cp.start()
        down_copy(e).start()

    barrier = pltpu.get_barrier_semaphore()
    writers = [{'eo': y, 'em': x, 'ei': 1 - c}]
    for j in range(1, n):
        writers += [{'eo': wrap(y + j * (1 - along_y)), 'em': wrap(x + j * along_y), 'ei': cc} for cc in range(cores)]
        writers.append(ahead(j))
    for device in writers:
        pl.semaphore_signal(barrier, inc=1, device_id=device, device_id_type=MESH)

    for cp in loads:
        cp.wait()
    slot = slot_ref[...]
    packed[...] = jnp.zeros_like(packed)
    packed[0:top] = jnp.where(slot >= 0, expert_ref[...] * slots + slot, -1).astype(jnp.float32)
    packed[ROUTE_ROWS:ROUTE_ROWS + top] = gate_ref[...]

    def route_send(step):
        return pltpu.make_async_remote_copy(
            src_ref=packed, dst_ref=routes.at[step - 1], send_sem=s3.at[step - 1], recv_sem=r3.at[step - 1],
            device_id=ahead(n - step), device_id_type=MESH)

    def wait_x(first, count):
        for b in range(count):
            pltpu.make_async_copy(x_hbm.at[0], xs.at[first + b], x_sem.at[first + b]).wait()

    def arrange_pair(p):
        wait_x(p * blocks, blocks)
        for k in range(0, model, TILE):
            cols = pl.ds(k, TILE)
            for b in range(part_blocks):
                first, second = (xs[p * blocks + 2 * b + h, :, cols].astype(jnp.float32) for h in range(2))
                for e in range(experts):
                    part_rows = slice(e * slots, (e + 1) * slots)
                    xe[e, p, pl.ds(b * rows, rows), cols] = jnp.concatenate(
                        [first[part_rows], second[part_rows]], axis=0).astype(jnp.bfloat16)

    def arrange_single(i):
        wait_x(i * blocks, blocks)
        for k in range(0, model, TILE):
            cols = pl.ds(k, TILE)
            for b in range(0, blocks, 2):
                first, second = (xs[i * blocks + b + h, :, cols].astype(jnp.float32) for h in range(2))
                for e in range(experts):
                    part_rows = slice(e * slots, (e + 1) * slots)
                    xe[e, 0, pl.ds(b * slots, rows), cols] = jnp.concatenate(
                        [first[part_rows], second[part_rows]], axis=0).astype(jnp.bfloat16)

    def gate_up(e, p, k, at):
        dst = pl.ds(at, blocks * slots)
        lhs = xe[e, p]
        if k < main_tiles:
            cols = pl.ds(k * TILE, TILE)
            g = jnp.dot(lhs, wg[e, :, cols], preferred_element_type=jnp.float32)
            u = jnp.dot(lhs, wu[e, :, cols], preferred_element_type=jnp.float32)
            hid[dst, cols] = (jax.nn.silu(g) * u).astype(jnp.bfloat16)
        else:
            gu = jnp.dot(lhs, wl[e], preferred_element_type=jnp.float32)
            hid[dst, pl.ds(ff_main, half)] = (jax.nn.silu(gu[:, :half]) * gu[:, half:]).astype(jnp.bfloat16)

    def down_pair(e, p, k):
        cols = pl.ds(k, DOWN_TILE)
        out = jnp.dot(hid[0:blocks * slots], wd[e, :, cols], preferred_element_type=jnp.float32).astype(jnp.bfloat16)
        ybuf[e, pl.ds(p * part_blocks, part_blocks), :, cols] = out.reshape(part_blocks, rows, DOWN_TILE)

    def down_single(s, k):
        cols = pl.ds(k, TILE)
        outs = [jnp.dot(hid[pl.ds(e * blocks * slots, blocks * slots)], wd[e, :, cols],
                        preferred_element_type=jnp.float32) for e in range(experts)]
        for b in range(blocks):
            block = jnp.concatenate([v[b * slots:(b + 1) * slots] for v in outs], axis=0)
            ybuf[s, b, :, cols] = block.astype(jnp.bfloat16)

    def row_sends(s, where):
        out = []
        for p in where:
            t, j = ORDER[p]
            if j and t == 0:
                out.append(pltpu.make_async_remote_copy(
                    src_ref=ybuf.at[s, p], dst_ref=recv.at[s, x, c], send_sem=s1.at[s, p],
                    recv_sem=r1.at[s, x, c], device_id={'eo': y, 'em': wrap(x + j), 'ei': 0}, device_id_type=MESH))
            elif j:
                out.append(pltpu.make_async_remote_copy(
                    src_ref=ybuf.at[s, p], dst_ref=recv.at[s, y, c], send_sem=s1.at[s, p],
                    recv_sem=r1.at[s, y, c], device_id={'eo': wrap(y + j), 'em': x, 'ei': 1}, device_id_type=MESH))
        if blocks - 1 in where:
            p = blocks - 1 - c
            q = jnp.where(c == 0, y, x)
            out.append(pltpu.make_async_remote_copy(
                src_ref=ybuf.at[s, p], dst_ref=recv.at[s, q, c], send_sem=s1.at[s, p],
                recv_sem=r1.at[s, q, c], device_id={'eo': y, 'em': x, 'ei': 1 - c}, device_id_type=MESH))
        return out

    near, far = range(part_blocks), range(part_blocks, blocks)

    def send_rows(s, where):
        for cp in row_sends(s, where):
            cp.start()
        if blocks - 1 in where:
            recv[s, ring, c] = ybuf[s, blocks - 2 + c]

    def wait_rows(s):
        def one(q, cc):
            pltpu.make_async_remote_copy(
                src_ref=ybuf.at[s, 0], dst_ref=recv.at[s, q, cc], send_sem=s1.at[s, 0],
                recv_sem=r1.at[s, q, cc], device_id={'eo': y, 'em': x, 'ei': 1 - c},
                device_id_type=MESH).wait_recv()
        one(ring, 1 - c)
        for j in range(1, n):
            for cc in range(cores):
                one(wrap(ring + j), cc)

    ways = (1, n - 1)

    def middle_send(h):
        return pltpu.make_async_remote_copy(
            src_ref=part.at[2, h], dst_ref=mid_in.at[h], send_sem=s4.at[h], recv_sem=r4.at[h],
            device_id=ahead(ways[h]), device_id_type=MESH)

    def part_send(way, h):
        return pltpu.make_async_remote_copy(
            src_ref=part.at[ways[way], h], dst_ref=prec.at[way, h], send_sem=s2.at[way, h], recv_sem=r2.at[way, h],
            device_id=ahead(ways[way]), device_id_type=MESH)

    def finish_part(way):
        middle_send(way).wait_recv()
        part[ways[way], way] = part[ways[way], way] + mid_in[way]
        part_send(way, way).start()

    def combine(step, order):
        route = routes[step - 1] if step else packed[...]
        chip = cores * experts
        base = jnp.where(c == 0, y * (n * chip), x * chip)
        jump = jnp.where(c == 0, chip, n * chip)
        row = lax.broadcasted_iota(jnp.int32, (slots, tokens), 0)
        weights, live = [], []
        for _, q, cc, e, _ in order:
            expert = base + q * jump + cc * experts + e
            key = (row + expert * slots).astype(jnp.float32)
            w = jnp.zeros((slots, tokens), jnp.float32)
            for j in range(top):
                w = w + jnp.where(route[j:j + 1, :] == key, route[ROUTE_ROWS + j:ROUTE_ROWS + j + 1, :], 0.0)
            weights.append(w)
            live.append(jnp.max(w, axis=1, keepdims=True) > 0)
        weight = jnp.concatenate(weights, axis=0)
        hi = weight.astype(jnp.bfloat16)
        rest = weight - hi.astype(jnp.float32)
        mid = rest.astype(jnp.bfloat16)
        low = (rest - mid.astype(jnp.float32)).astype(jnp.bfloat16)
        lhs = jnp.concatenate([hi, mid, low], axis=1)
        for k in range(down_tiles):
            cols = pl.ds(k * TILE, TILE)
            got = []
            for (s, q, cc, _, at), keep in zip(order, live):
                block = recv[s, q, cc, :, cols].astype(jnp.float32)
                got.append(jnp.where(keep, block[at * slots:(at + 1) * slots], 0.0))
            got = jnp.concatenate(got, axis=0).astype(jnp.bfloat16)
            p = lax.dot_general(lhs, got, (((0,), (0,)), ((), ())), preferred_element_type=jnp.float32)
            part[step, k // (down_tiles // 2), :, pl.ds(k % (down_tiles // 2) * TILE, TILE)] = (
                (p[2 * tokens:] + p[tokens:2 * tokens]) + p[:tokens])

    senders = [(q, cc) for q in range(n) for cc in range(cores)]

    @pl.loop(0, 2 * experts)
    def _(u):
        e, p = u // 2, lax.rem(u, 2)

        @pl.when(u < 2)
        def _():
            arrange_pair(p)

        @pl.when(u == 1)
        def _():
            for i in range(2):
                for cp in single_copies(i):
                    cp.start()

        for m in range(experts):
            @pl.when(u == 2 * m)
            def _():
                for cp in gate_up_copies(m):
                    cp.wait()
        for k in range(main_tiles + 1):
            gate_up(e, p, k, 0)
        for m in range(experts):
            @pl.when(u == 2 * m)
            def _():
                down_copy(m).wait()
        for k in range(0, model, DOWN_TILE):
            down_pair(e, p, k)

        @pl.when(u == 0)
        def _():
            pl.semaphore_wait(barrier, len(writers))
            for step in range(1, n):
                route_send(step).start()

        @pl.when(p == 0)
        def _():
            send_rows(e, near)

        @pl.when(p == 1)
        def _():
            send_rows(e, far)

    @pl.loop(experts, stages)
    def _(s):
        arrange_single(s - experts)
        for e in range(experts):
            for k in range(main_tiles + 1):
                gate_up(e, 0, k, e * blocks * slots)
        for k in range(0, model, TILE):
            down_single(s, k)
        send_rows(s, range(blocks))

        @pl.when(s == experts)
        def _():
            for step in range(1, n):
                route_send(step).wait_recv()
            for e in range(experts):
                wait_rows(e)
            for h in range(2):
                combine(PAIR[h], [(e, q, cc, e, h) for e in range(experts) for q, cc in senders])
                if h == 0:
                    for way in range(2):
                        middle_send(way).start()
                else:
                    part_send(0, 1).start()

    finish_part(0)
    for i in range(2):
        wait_rows(experts + i)
        combine(SINGLE[i], [(experts + i, q, cc, e, e) for q, cc in senders for e in range(experts)])
        if i == 0:
            part_send(1, 0).start()
            finish_part(1)
    for h in range(2):
        for way in range(2):
            part_send(way, h).wait_recv()
        for k in range(0, model // 2, TILE):
            cols = pl.ds(k, TILE)
            total = part[0, h, :, cols] + prec[0, h, :, cols] + prec[1, h, :, cols]
            out_ref[:, pl.ds(h * (model // 2) + k, TILE)] = total.astype(out_ref.dtype)
    for way in range(2):
        middle_send(way).wait_send()
        for h in range(2):
            part_send(way, h).wait_send()
    for step in range(1, n):
        route_send(step).wait_send()

    @pl.loop(0, stages)
    def _(s):
        for cp in row_sends(s, range(blocks)):
            cp.wait_send()


def solution(mesh):
    token_spec = P(('dp',) + GROUP_AXES, None)
    weight_spec = P(GROUP_AXES, None, None)
    rows_spec = P('dp', GROUP_AXES, None, None)
    n, cores = mesh.shape['eo'], mesh.shape['ei']
    assert mesh.shape['em'] == n == 4 and cores == 2

    def local_part(x_local, w_gate, w_up, w_down, slot_idx, expert_idx, gate_wt):
        sources, experts, slots, model = x_local.shape
        ff = w_gate.shape[2]
        tokens, top = slot_idx.shape
        ff_main = ff // TILE * TILE
        half = ff - ff_main
        assert 2 * half == TILE and experts == 2
        rows = 2 * slots
        blocks = 2 * n
        stages = 2 * experts
        hbm = pl.BlockSpec(memory_space=pl.ANY)
        vmem = pl.BlockSpec(memory_space=pltpu.VMEM)
        dma = pltpu.SemaphoreType.DMA
        return pl.pallas_call(
            functools.partial(kernel, n, cores, slots, top),
            out_shape=jax.ShapeDtypeStruct((tokens, model), jnp.bfloat16),
            in_specs=[hbm] * 7,
            out_specs=vmem,
            scratch_shapes=[
                pltpu.VMEM((experts, model, ff_main), jnp.bfloat16),
                pltpu.VMEM((experts, model, ff_main), jnp.bfloat16),
                pltpu.VMEM((experts, model, 2 * half), jnp.bfloat16),
                pltpu.VMEM((experts, ff, model), jnp.bfloat16),
                pltpu.VMEM((2 * blocks, experts * slots, model), jnp.bfloat16),
                pltpu.VMEM((experts, 2, blocks * slots, model), jnp.bfloat16),
                pltpu.VMEM((experts * blocks * slots, ff), jnp.bfloat16),
                pltpu.VMEM((stages, blocks, rows, model), jnp.bfloat16),
                pltpu.VMEM((stages, n, cores, rows, model), jnp.bfloat16),
                pltpu.VMEM((n, 2, tokens, model // 2), jnp.float32),
                pltpu.VMEM((2, tokens, model // 2), jnp.float32),
                pltpu.VMEM((2, 2, tokens, model // 2), jnp.float32),
                pltpu.VMEM((top, tokens), jnp.int32),
                pltpu.VMEM((top, tokens), jnp.int32),
                pltpu.VMEM((top, tokens), jnp.float32),
                pltpu.VMEM((2 * ROUTE_ROWS, tokens), jnp.float32),
                pltpu.VMEM((n - 1, 2 * ROUTE_ROWS, tokens), jnp.float32),
                dma((experts, 2)), dma((experts, 2)), dma((experts,)), dma((2 * blocks,)), dma((3,)),
                dma((stages, blocks)), dma((stages, n, cores)), dma((2, 2)), dma((2, 2)), dma((n - 1,)), dma((n - 1,)), dma((2,)), dma((2,)),
            ],
            compiler_params=pltpu.CompilerParams(
                collective_id=0, has_side_effects=True, vmem_limit_bytes=67_000_000),
        )(x_local.reshape(sources, experts * slots, model), w_gate, w_up, w_down, slot_idx.T, expert_idx.T, gate_wt.T)

    return jax.shard_map(local_part, mesh=mesh,
                         in_specs=(rows_spec, weight_spec, weight_spec, weight_spec, token_spec, token_spec, token_spec),
                         out_specs=token_spec, check_vma=False)
```

```python
import functools

import jax
import jax.numpy as jnp
from jax import lax
from jax.experimental import pallas as pl
from jax.experimental.pallas import tpu as pltpu
from jax.sharding import PartitionSpec as P

GROUP_AXES = ('eo', 'em', 'ei')
MESH = pl.DeviceIdType.MESH
TILE = 256
DOWN_TILE = 512
ROUTE_ROWS = 8
PAIR = (2, 1)
SINGLE = (3, 0)
ORDER = ((0, 2), (1, 2), (0, 1), (1, 1), (0, 3), (1, 3), (0, 0), (1, 0))


def kernel(n, cores, slots, top, x_hbm, wg_hbm, wu_hbm, wd_hbm, slot_hbm, expert_hbm, gate_hbm, out_ref,
           wg, wu, wl, wd, xs, xe, hid, ybuf, recv, part, mid_in, prec, slot_ref, expert_ref, gate_ref, packed, routes,
           gu_sem, wl_sem, wd_sem, x_sem, route_sem, s1, r1, s2, r2, s3, r3, s4, r4):
    experts, model, ff = wg_hbm.shape
    ff_main = wg.shape[2]
    half = ff - ff_main
    rows = 2 * slots
    blocks = 2 * n
    part_blocks = blocks // 2
    stages = 2 * experts
    tokens = out_ref.shape[0]
    y, x, c = (lax.axis_index(a) for a in GROUP_AXES)
    ring = jnp.where(c == 0, x, y)
    along_y = jnp.where(c == 0, 1, 0)

    def wrap(v):
        return lax.rem(v, n)

    def ahead(step):
        return {'eo': wrap(y + step * along_y), 'em': wrap(x + step * (1 - along_y)), 'ei': c}

    def x_copy(t, j, step, d):
        if t == 0:
            src = (wrap(y + step) * n + wrap(x + j)) * cores
        else:
            src = (wrap(y + j) * n + wrap(x + step)) * cores + 1
        return pltpu.make_async_copy(x_hbm.at[src], xs.at[d], x_sem.at[d])

    def pair_copies():
        return [x_copy(t, j, PAIR[h], 2 * p + h) for p, (t, j) in enumerate(ORDER) for h in range(2)]

    def single_copies(i):
        return [x_copy(t, j, SINGLE[i], i * blocks + p) for p, (t, j) in enumerate(ORDER)]

    main_tiles = ff_main // TILE
    down_tiles = model // TILE

    def gate_up_copies(e):
        out = []
        for a, (w, v) in enumerate(((wg_hbm, wg), (wu_hbm, wu))):
            out.append(pltpu.make_async_copy(w.at[e, :, pl.ds(0, ff_main)], v.at[e], gu_sem.at[e, a]))
            out.append(pltpu.make_async_copy(
                w.at[e, :, pl.ds(ff_main, half)], wl.at[e, :, pl.ds(a * half, half)], wl_sem.at[e, a]))
        return out

    def down_copy(e):
        return pltpu.make_async_copy(wd_hbm.at[e], wd.at[e], wd_sem.at[e])

    loads = [pltpu.make_async_copy(src, dst, route_sem.at[i]) for i, (src, dst) in enumerate(
        ((slot_hbm, slot_ref), (expert_hbm, expert_ref), (gate_hbm, gate_ref)))]
    for cp in loads:
        cp.start()
    for cp in pair_copies():
        cp.start()
    for e in range(experts):
        for cp in gate_up_copies(e):
            cp.start()
        down_copy(e).start()

    barrier = pltpu.get_barrier_semaphore()
    writers = [{'eo': y, 'em': x, 'ei': 1 - c}]
    for j in range(1, n):
        writers += [{'eo': wrap(y + j * (1 - along_y)), 'em': wrap(x + j * along_y), 'ei': cc} for cc in range(cores)]
        writers.append(ahead(j))
    for device in writers:
        pl.semaphore_signal(barrier, inc=1, device_id=device, device_id_type=MESH)

    for cp in loads:
        cp.wait()
    slot = slot_ref[...]
    packed[...] = jnp.zeros_like(packed)
    packed[0:top] = jnp.where(slot >= 0, expert_ref[...] * slots + slot, -1).astype(jnp.float32)
    packed[ROUTE_ROWS:ROUTE_ROWS + top] = gate_ref[...]

    def route_send(step):
        return pltpu.make_async_remote_copy(
            src_ref=packed, dst_ref=routes.at[step - 1], send_sem=s3.at[step - 1], recv_sem=r3.at[step - 1],
            device_id=ahead(n - step), device_id_type=MESH)

    def wait_x(first, count):
        for b in range(count):
            pltpu.make_async_copy(x_hbm.at[0], xs.at[first + b], x_sem.at[first + b]).wait()

    def arrange_pair(p):
        wait_x(p * blocks, blocks)
        for k in range(0, model, TILE):
            cols = pl.ds(k, TILE)
            for b in range(part_blocks):
                first, second = (xs[p * blocks + 2 * b + h, :, cols].astype(jnp.float32) for h in range(2))
                for e in range(experts):
                    part_rows = slice(e * slots, (e + 1) * slots)
                    xe[e, p, pl.ds(b * rows, rows), cols] = jnp.concatenate(
                        [first[part_rows], second[part_rows]], axis=0).astype(jnp.bfloat16)

    def arrange_single(i):
        wait_x(i * blocks, blocks)
        for k in range(0, model, TILE):
            cols = pl.ds(k, TILE)
            for b in range(0, blocks, 2):
                first, second = (xs[i * blocks + b + h, :, cols].astype(jnp.float32) for h in range(2))
                for e in range(experts):
                    part_rows = slice(e * slots, (e + 1) * slots)
                    xe[e, 0, pl.ds(b * slots, rows), cols] = jnp.concatenate(
                        [first[part_rows], second[part_rows]], axis=0).astype(jnp.bfloat16)

    def gate_up(e, p, k, at):
        dst = pl.ds(at, blocks * slots)
        lhs = xe[e, p]
        if k < main_tiles:
            cols = pl.ds(k * TILE, TILE)
            g = jnp.dot(lhs, wg[e, :, cols], preferred_element_type=jnp.float32)
            u = jnp.dot(lhs, wu[e, :, cols], preferred_element_type=jnp.float32)
            hid[dst, cols] = (jax.nn.silu(g) * u).astype(jnp.bfloat16)
        else:
            gu = jnp.dot(lhs, wl[e], preferred_element_type=jnp.float32)
            hid[dst, pl.ds(ff_main, half)] = (jax.nn.silu(gu[:, :half]) * gu[:, half:]).astype(jnp.bfloat16)

    def down_pair(e, p, k):
        cols = pl.ds(k, DOWN_TILE)
        out = jnp.dot(hid[0:blocks * slots], wd[e, :, cols], preferred_element_type=jnp.float32).astype(jnp.bfloat16)
        ybuf[e, pl.ds(p * part_blocks, part_blocks), :, cols] = out.reshape(part_blocks, rows, DOWN_TILE)

    def down_single(s, k):
        cols = pl.ds(k, TILE)
        outs = [jnp.dot(hid[pl.ds(e * blocks * slots, blocks * slots)], wd[e, :, cols],
                        preferred_element_type=jnp.float32) for e in range(experts)]
        for b in range(blocks):
            block = jnp.concatenate([v[b * slots:(b + 1) * slots] for v in outs], axis=0)
            ybuf[s, b, :, cols] = block.astype(jnp.bfloat16)

    def row_sends(s, where):
        out = []
        for p in where:
            t, j = ORDER[p]
            if j and t == 0:
                out.append(pltpu.make_async_remote_copy(
                    src_ref=ybuf.at[s, p], dst_ref=recv.at[s, x, c], send_sem=s1.at[s, p],
                    recv_sem=r1.at[s, x, c], device_id={'eo': y, 'em': wrap(x + j), 'ei': 0}, device_id_type=MESH))
            elif j:
                out.append(pltpu.make_async_remote_copy(
                    src_ref=ybuf.at[s, p], dst_ref=recv.at[s, y, c], send_sem=s1.at[s, p],
                    recv_sem=r1.at[s, y, c], device_id={'eo': wrap(y + j), 'em': x, 'ei': 1}, device_id_type=MESH))
        if blocks - 1 in where:
            p = blocks - 1 - c
            q = jnp.where(c == 0, y, x)
            out.append(pltpu.make_async_remote_copy(
                src_ref=ybuf.at[s, p], dst_ref=recv.at[s, q, c], send_sem=s1.at[s, p],
                recv_sem=r1.at[s, q, c], device_id={'eo': y, 'em': x, 'ei': 1 - c}, device_id_type=MESH))
        return out

    near, far = range(part_blocks), range(part_blocks, blocks)

    def send_rows(s, where):
        for cp in row_sends(s, where):
            cp.start()
        if blocks - 1 in where:
            recv[s, ring, c] = ybuf[s, blocks - 2 + c]

    def wait_rows(s):
        def one(q, cc):
            pltpu.make_async_remote_copy(
                src_ref=ybuf.at[s, 0], dst_ref=recv.at[s, q, cc], send_sem=s1.at[s, 0],
                recv_sem=r1.at[s, q, cc], device_id={'eo': y, 'em': x, 'ei': 1 - c},
                device_id_type=MESH).wait_recv()
        one(ring, 1 - c)
        for j in range(1, n):
            for cc in range(cores):
                one(wrap(ring + j), cc)

    ways = (1, n - 1)

    def middle_send(h):
        return pltpu.make_async_remote_copy(
            src_ref=part.at[2, h], dst_ref=mid_in.at[h], send_sem=s4.at[h], recv_sem=r4.at[h],
            device_id=ahead(ways[h]), device_id_type=MESH)

    def part_send(way, h):
        return pltpu.make_async_remote_copy(
            src_ref=part.at[ways[way], h], dst_ref=prec.at[way, h], send_sem=s2.at[way, h], recv_sem=r2.at[way, h],
            device_id=ahead(ways[way]), device_id_type=MESH)

    def finish_part(way):
        middle_send(way).wait_recv()
        part[ways[way], way] = part[ways[way], way] + mid_in[way]
        part_send(way, way).start()

    def combine(step, order):
        route = routes[step - 1] if step else packed[...]
        chip = cores * experts
        base = jnp.where(c == 0, y * (n * chip), x * chip)
        jump = jnp.where(c == 0, chip, n * chip)
        row = lax.broadcasted_iota(jnp.int32, (slots, tokens), 0)
        weights, live = [], []
        for _, q, cc, e, _ in order:
            expert = base + q * jump + cc * experts + e
            key = (row + expert * slots).astype(jnp.float32)
            w = jnp.zeros((slots, tokens), jnp.float32)
            for j in range(top):
                w = w + jnp.where(route[j:j + 1, :] == key, route[ROUTE_ROWS + j:ROUTE_ROWS + j + 1, :], 0.0)
            weights.append(w)
            live.append(jnp.max(w, axis=1, keepdims=True) > 0)
        weight = jnp.concatenate(weights, axis=0)
        hi = weight.astype(jnp.bfloat16)
        rest = weight - hi.astype(jnp.float32)
        mid = rest.astype(jnp.bfloat16)
        low = (rest - mid.astype(jnp.float32)).astype(jnp.bfloat16)
        lhs = jnp.concatenate([hi, mid, low], axis=1)
        for k in range(down_tiles):
            cols = pl.ds(k * TILE, TILE)
            got = []
            for (s, q, cc, _, at), keep in zip(order, live):
                block = recv[s, q, cc, :, cols].astype(jnp.float32)
                got.append(jnp.where(keep, block[at * slots:(at + 1) * slots], 0.0))
            got = jnp.concatenate(got, axis=0).astype(jnp.bfloat16)
            p = lax.dot_general(lhs, got, (((0,), (0,)), ((), ())), preferred_element_type=jnp.float32)
            part[step, k // (down_tiles // 2), :, pl.ds(k % (down_tiles // 2) * TILE, TILE)] = (
                (p[2 * tokens:] + p[tokens:2 * tokens]) + p[:tokens])

    senders = [(q, cc) for q in range(n) for cc in range(cores)]

    @pl.loop(0, 2 * experts)
    def _(u):
        e, p = u // 2, lax.rem(u, 2)

        @pl.when(u < 2)
        def _():
            arrange_pair(p)

        @pl.when(u == 1)
        def _():
            for i in range(2):
                for cp in single_copies(i):
                    cp.start()

        for m in range(experts):
            @pl.when(u == 2 * m)
            def _():
                for cp in gate_up_copies(m):
                    cp.wait()
        for k in range(main_tiles + 1):
            gate_up(e, p, k, 0)
        for m in range(experts):
            @pl.when(u == 2 * m)
            def _():
                down_copy(m).wait()
        for k in range(0, model, DOWN_TILE):
            down_pair(e, p, k)

        @pl.when(u == 0)
        def _():
            pl.semaphore_wait(barrier, len(writers))
            for step in range(1, n):
                route_send(step).start()

        @pl.when(p == 0)
        def _():
            send_rows(e, near)

        @pl.when(p == 1)
        def _():
            send_rows(e, far)

    @pl.loop(experts, stages)
    def _(s):
        arrange_single(s - experts)
        for e in range(experts):
            for k in range(main_tiles + 1):
                gate_up(e, 0, k, e * blocks * slots)
        for k in range(0, model, TILE):
            down_single(s, k)
        send_rows(s, range(blocks))

        @pl.when(s == experts)
        def _():
            for step in range(1, n):
                route_send(step).wait_recv()
            for e in range(experts):
                wait_rows(e)
            for h in range(2):
                combine(PAIR[h], [(e, q, cc, e, h) for e in range(experts) for q, cc in senders])
                if h == 0:
                    for way in range(2):
                        middle_send(way).start()
                else:
                    part_send(0, 1).start()

    finish_part(0)
    for i in range(2):
        wait_rows(experts + i)
        combine(SINGLE[i], [(experts + i, q, cc, e, e) for q, cc in senders for e in range(experts)])
        if i == 0:
            part_send(1, 0).start()
            finish_part(1)
    for h in range(2):
        for way in range(2):
            part_send(way, h).wait_recv()
        for k in range(0, model // 2, TILE):
            cols = pl.ds(k, TILE)
            total = part[0, h, :, cols] + prec[0, h, :, cols] + prec[1, h, :, cols]
            out_ref[:, pl.ds(h * (model // 2) + k, TILE)] = total.astype(out_ref.dtype)
    for way in range(2):
        middle_send(way).wait_send()
        for h in range(2):
            part_send(way, h).wait_send()
    for step in range(1, n):
        route_send(step).wait_send()

    @pl.loop(0, stages)
    def _(s):
        for cp in row_sends(s, range(blocks)):
            cp.wait_send()


def solution(mesh):
    token_spec = P(('dp',) + GROUP_AXES, None)
    weight_spec = P(GROUP_AXES, None, None)
    rows_spec = P('dp', GROUP_AXES, None, None)
    n, cores = mesh.shape['eo'], mesh.shape['ei']
    assert mesh.shape['em'] == n == 4 and cores == 2

    def local_part(x_local, w_gate, w_up, w_down, slot_idx, expert_idx, gate_wt):
        sources, experts, slots, model = x_local.shape
        ff = w_gate.shape[2]
        tokens, top = slot_idx.shape
        ff_main = ff // TILE * TILE
        half = ff - ff_main
        assert 2 * half == TILE and experts == 2
        rows = 2 * slots
        blocks = 2 * n
        stages = 2 * experts
        hbm = pl.BlockSpec(memory_space=pl.ANY)
        vmem = pl.BlockSpec(memory_space=pltpu.VMEM)
        dma = pltpu.SemaphoreType.DMA
        return pl.pallas_call(
            functools.partial(kernel, n, cores, slots, top),
            out_shape=jax.ShapeDtypeStruct((tokens, model), jnp.bfloat16),
            in_specs=[hbm] * 7,
            out_specs=vmem,
            scratch_shapes=[
                pltpu.VMEM((experts, model, ff_main), jnp.bfloat16),
                pltpu.VMEM((experts, model, ff_main), jnp.bfloat16),
                pltpu.VMEM((experts, model, 2 * half), jnp.bfloat16),
                pltpu.VMEM((experts, ff, model), jnp.bfloat16),
                pltpu.VMEM((2 * blocks, experts * slots, model), jnp.bfloat16),
                pltpu.VMEM((experts, 2, blocks * slots, model), jnp.bfloat16),
                pltpu.VMEM((experts * blocks * slots, ff), jnp.bfloat16),
                pltpu.VMEM((stages, blocks, rows, model), jnp.bfloat16),
                pltpu.VMEM((stages, n, cores, rows, model), jnp.bfloat16),
                pltpu.VMEM((n, 2, tokens, model // 2), jnp.float32),
                pltpu.VMEM((2, tokens, model // 2), jnp.float32),
                pltpu.VMEM((2, 2, tokens, model // 2), jnp.float32),
                pltpu.VMEM((top, tokens), jnp.int32),
                pltpu.VMEM((top, tokens), jnp.int32),
                pltpu.VMEM((top, tokens), jnp.float32),
                pltpu.VMEM((2 * ROUTE_ROWS, tokens), jnp.float32),
                pltpu.VMEM((n - 1, 2 * ROUTE_ROWS, tokens), jnp.float32),
                dma((experts, 2)), dma((experts, 2)), dma((experts,)), dma((2 * blocks,)), dma((3,)),
                dma((stages, blocks)), dma((stages, n, cores)), dma((2, 2)), dma((2, 2)), dma((n - 1,)), dma((n - 1,)), dma((2,)), dma((2,)),
            ],
            compiler_params=pltpu.CompilerParams(
                collective_id=0, has_side_effects=True, vmem_limit_bytes=67_000_000),
        )(x_local.reshape(sources, experts * slots, model), w_gate, w_up, w_down, slot_idx.T, expert_idx.T, gate_wt.T)

    return jax.shard_map(local_part, mesh=mesh,
                         in_specs=(rows_spec, weight_spec, weight_spec, weight_spec, token_spec, token_spec, token_spec),
                         out_specs=token_spec, check_vma=False)
```
